256 devices in a mesh: block: 4 (over y), tok: 64 (over z, x, core).
Axes of the slice: x: 4, y: 4, z: 8, core: 2. Of those that a mesh axis runs over, the one named last changes fastest.
Arguments:
- queries: float32 [32768, 256], P(('block', 'tok')), may hold values from -6 to 6
- keys: float32 [32768, 256], P(('block', 'tok')), may hold values from -6 to 6
- values: float32 [32768, 256], P(('block', 'tok')), may hold values from -6 to 6
- rates: float32 [32768], P(('block', 'tok')), may hold values from 0.0001 to 0.001
- states: float32 [4, 3, 256, 256], P('block', None, 'tok'), may hold values from -0.375 to 0.375
- out_cot: float32 [32768, 256], P(('block', 'tok')), may hold values from -6 to 6
- final_cot: float32 [3, 256, 256], P(None, 'tok'), may hold values from -6 to 6
Outputs:
- d_queries: float32 [32768, 256], P(('block', 'tok'))
- d_keys: float32 [32768, 256], P(('block', 'tok'))
- d_values: float32 [32768, 256], P(('block', 'tok'))
- d_rates: float32 [32768], P(('block', 'tok'))
- d_states: float32 [4, 3, 256, 256], P('block', None, 'tok')
The draws below stay inside these ranges and needn't reach their ends.
All inputs are finite; a program needn't handle non-finite values.
Results may differ from the reference program's by a relative error of at most 0.00029.
Values sent between devices are 32-bit elements; how exact they have to be, the bound alone decides.
A program may use at most 64 MiB of HBM per device.

```python
import math
import jax
import jax.numpy as jnp
from jax import lax

D = 256
TOKENS = 32768
N_BLOCK = 4


def block_levels(key, dims, pieces, low, largest):
    gain, own = 1.0, jax.random.fold_in(key, 6)
    for dim, parts in pieces:
        heights = jnp.exp(jax.random.uniform(jax.random.fold_in(own, dim), (parts,), jnp.float32, low / len(pieces), largest / len(pieces)))
        gain = gain * jnp.repeat(heights, dims[dim] // parts).reshape([-1 if axis == dim else 1 for axis in range(len(dims))])
    return gain


def bell_draw(key, extent, scale, bound, cuts=(), dtype=jnp.bfloat16):
    gain = block_levels(key, extent, cuts, -0.22, 0.18) if cuts else 1.0
    entries = jax.random.normal(key, extent, jnp.float32) * scale * gain
    return jnp.minimum(jnp.maximum(entries, -bound), bound).astype(dtype)


def setup_inputs(seed: int = 0) -> dict:
    key_list = jax.random.split(jax.random.key(seed), 8)
    queries = bell_draw(key_list[0], (TOKENS, D), 1.0, 6.0, ((0, 256),), jnp.float32)
    keys = bell_draw(key_list[1], (TOKENS, D), 1.0, 6.0, ((0, 256),), jnp.float32)
    values = bell_draw(key_list[2], (TOKENS, D), 1.0, 6.0, ((0, 256),), jnp.float32)
    rates = jnp.clip(jnp.exp(math.log(0.001) - 2.3025852 * jax.random.uniform(key_list[3], (TOKENS,), jnp.float32) ** block_levels(key_list[3], (TOKENS,), ((0, 256),), -0.2, 0.2)), 0.0001, 0.001)
    states = bell_draw(key_list[4], (N_BLOCK, 3, D, D), D ** -0.5, 0.375, ((0, 4), (2, 64)), jnp.float32)
    out_cot = bell_draw(key_list[5], (TOKENS, D), 1.0, 6.0, ((0, 256),), jnp.float32)
    final_cot = bell_draw(key_list[6], (3, D, D), 1.0, 6.0, ((1, 64),), jnp.float32)
    return dict(queries=queries, keys=keys, values=values, rates=rates, states=states, out_cot=out_cot, final_cot=final_cot)


EPS = 1e-06
HIGH = lax.Precision.HIGHEST

def apply_fast(weights, inputs):
    first = jnp.dot(inputs, weights[0], precision=HIGH, preferred_element_type=jnp.float32)
    gate = jnp.dot(inputs, weights[1], precision=HIGH, preferred_element_type=jnp.float32)
    mixed = jax.nn.silu(first) * gate
    return jnp.dot(mixed, weights[2], precision=HIGH, preferred_element_type=jnp.float32)

def update_grad(weights, keys, values, rates):

    def loss(current):
        return -jnp.sum(rates[:, None] * apply_fast(current, keys) * values)
    return jax.grad(loss)(weights)

def renorm(weights, grads):
    shifted = weights - grads
    row_norm = jnp.sqrt(lax.optimization_barrier(jnp.sum(weights * weights, axis=-1, keepdims=True)) + EPS)
    new_norm = jnp.sqrt(lax.optimization_barrier(jnp.sum(shifted * shifted, axis=-1, keepdims=True)) + EPS)
    return shifted * (row_norm / new_norm)

def block_map(weights, queries, keys, values, rates):
    return (apply_fast(weights, queries), renorm(weights, update_grad(weights, keys, values, rates)))

def reference(queries, keys, values, rates, states, out_cot, final_cot):
    length = queries.shape[0] // N_BLOCK
    incoming = final_cot
    grad_q = [None] * N_BLOCK
    grad_k = [None] * N_BLOCK
    grad_v = [None] * N_BLOCK
    grad_r = [None] * N_BLOCK
    grad_s = [None] * N_BLOCK
    for index in range(N_BLOCK - 1, -1, -1):
        start = index * length
        stop = start + length
        _, backward = jax.vjp(block_map, states[index], queries[start:stop], keys[start:stop], values[start:stop], rates[start:stop])
        d_weights, d_q, d_k, d_v, d_r = backward((out_cot[start:stop], incoming))
        grad_q[index] = d_q
        grad_k[index] = d_k
        grad_v[index] = d_v
        grad_r[index] = d_r
        grad_s[index] = d_weights
        incoming = d_weights
    return (jnp.concatenate(grad_q, axis=0), jnp.concatenate(grad_k, axis=0), jnp.concatenate(grad_v, axis=0), jnp.concatenate(grad_r, axis=0), jnp.stack(grad_s, axis=0))
```

```python
import functools

import jax
import jax.numpy as jnp
from jax import lax
from jax.experimental import pallas as pl
from jax.experimental.pallas import tpu as pltpu
from jax.sharding import PartitionSpec as P

EPS = 1e-06
F32 = jnp.float32
BF16 = jnp.bfloat16
D = 256
HALF = 128
NZ, NX = 8, 4
NN = (((1,), (0,)), ((), ()))
NT = (((1,), (1,)), ((), ()))
TN = (((0,), (0,)), ((), ()))
FAR_FIRST = (4, 3, 5, 2, 6, 1, 7)
NEAR_FIRST = (0, 1, 7, 2, 6, 3, 5, 4)


def split(a):
    hi = a.astype(BF16)
    return hi, (a - hi.astype(F32)).astype(BF16)


def dot1(a, b, dims):
    return lax.dot_general(a, b, dims, preferred_element_type=F32)


def dot3(a, b, dims):
    return dot1(a[0], b[0], dims) + (dot1(a[0], b[1], dims) + dot1(a[1], b[0], dims))


def exact_select(a, one_hot):
    hi = a.astype(BF16)
    rest = a - hi.astype(F32)
    mid = rest.astype(BF16)
    low = (rest - mid.astype(F32)).astype(BF16)
    return (dot1(hi, one_hot, NN) + dot1(mid, one_hot, NN)) + dot1(low, one_hot, NN)


def silu_parts(u):
    sig = 1.0 / (1.0 + jnp.exp(-u))
    return sig, u * sig, sig * (1.0 + u * (1.0 - sig))


def kernel(
    q_in, k_in, v_in, r_in, s_in, oc_in, fc_in,
    dq_out, dk_out, dv_out, dr_out, ds_out,
    k_sib, v_sib, q_sib, oc_sib, r_own, r_sib,
    own_w, own_z, rows_z, z_in, nat,
    g_w, g_d, p_g, p_z, rx_g, rx_z, rza_g, rzb_g, rza_z, rzb_z, sum_g, sum_z,
    w13, w2, d13, d2, ap13, ap2, t13, t2,
    kh, kl, kth, ktl, vh, vl,
    w13h, w13l, w2h, w2l, d13h, d13l, d2h, d2l,
    c_uu, c_ug, c_uq, c_gq, g_ug, g_q, a_ug, a_q,
    part_q, part_k, part_v, part_r, fin_q, fin_k, fin_v, fin_r,
    sib_s, sib_r,
    agw_s, agw_za, agw_zb, agw_x, agd_s, agd_za, agd_zb, agd_x,
    rsg_s, rsg_x, rsg_z, rsz_s, rsz_x, rsz_z,
    y_sem, fin_s, fin_r_sem,
):
    y = lax.axis_index("block")
    t = lax.axis_index("tok")
    core = lax.rem(t, 2)
    x = lax.rem(lax.div(t, 2), NX)
    z = lax.div(t, 2 * NX)

    def tok(zz, xx, cc):
        return (zz * NX + xx) * 2 + cc

    def ahead(a, by, n):
        return lax.rem(a + by, n)

    sibling = tok(z, x, 1 - core)

    def send(src, dst, s_sem, r_sem, to):
        pltpu.make_async_remote_copy(
            src_ref=src, dst_ref=dst, send_sem=s_sem, recv_sem=r_sem,
            device_id=(y, to), device_id_type=pl.DeviceIdType.MESH,
        ).start()

    def wait(ref, sem):
        pltpu.make_async_copy(ref, ref, sem).wait()

    barrier = pltpu.get_barrier_semaphore()

    def greet(block, to):
        pl.semaphore_signal(barrier, inc=1, device_id=(block, to), device_id_type=pl.DeviceIdType.MESH)

    for d in FAR_FIRST:
        greet(y, tok(ahead(z, d, NZ), x, core))
        greet(y, tok(ahead(z, d, NZ), x, 1 - core))
    for dx in (2, 1, 3):
        greet(y, tok(z, ahead(x, dx, NX), core))
    greet(y, sibling)
    greet(ahead(y, 1, 4), t)
    greet(ahead(y, 3, 4), t)

    row_i = lax.broadcasted_iota(jnp.int32, (D, D), 0)
    col_i = lax.broadcasted_iota(jnp.int32, (D, D), 1)

    def hidden_of(p):
        return 8 * ((p & 127) >> 2) + 4 * (p >> 7) + (p & 3)

    top = lax.broadcasted_iota(jnp.int32, (8, HALF), 0) < 4

    def half_swap(a):
        return pltpu.roll(a, 4, 0)

    def pick(first, second):
        return jnp.where(core == 0, first, second)

    def to_own(ref3, out):
        nat[0:4, :] = ref3[0]
        nat[4:8, :] = ref3[1]
        nat[8:12, :] = ref3[2]
        one_hot = (row_i == hidden_of(col_i)).astype(F32).astype(BF16)
        a = exact_select(nat[0:8, :], one_hot)
        out[0:8, :] = pick(a[:, :HALF], a[:, HALF:])
        out[16:24, :] = pick(a[:, HALF:], a[:, :HALF])
        b = nat[8:16, :]
        out[8:16, :] = jnp.where(top, b[:, :HALF], half_swap(b[:, HALF:]))

    nat[...] = jnp.zeros_like(nat)
    to_own(s_in.at[0], own_w)
    r_own[...] = jnp.broadcast_to(r_in[...], (8, HALF))

    pl.semaphore_wait(barrier, 20)

    pairs = ((k_in, k_sib), (v_in, v_sib), (q_in, q_sib), (oc_in, oc_sib), (r_own, r_sib))

    def share(n):
        send(pairs[n][0], pairs[n][1], sib_s.at[n], sib_r.at[n], sibling)

    def gather_start(own, g, sems, za, zb):
        g[x, z, 0:16, :] = own[0:16, :]
        for d in FAR_FIRST:
            zp = ahead(z, d, NZ)
            send(own.at[0:16], g.at[x, z, 0:16], sems.at[0], za.at[d], tok(zp, x, core))
            send(own.at[16:24], g.at[x, z, 16:24], sems.at[1], zb.at[d], tok(zp, x, 1 - core))
        send(own.at[16:24], g.at[x, z, 16:24], sems.at[1], zb.at[0], sibling)

    def gather_finish(g, sems, za, zb, xs):
        for d in NEAR_FIRST:
            zs = ahead(z, NZ - d, NZ)
            if d:
                wait(g.at[x, zs, 0:16], za.at[d])
            wait(g.at[x, zs, 16:24], zb.at[d])
            for dx in (2, 1, 3):
                send(g.at[x, zs], g.at[x, zs], sems.at[2], xs, tok(z, ahead(x, dx, NX), core))
        wait(g.at[0:3], xs)

    def gather_sent(g, sems):
        wait(rza_g, sems.at[0])
        wait(rzb_g, sems.at[1])
        wait(g.at[0:3], sems.at[2])

    def assemble(g, w13_ref, w2_ref):
        def step(zz, carry):
            for xx in range(NX):
                same, other = g[xx, zz, 0:8, :], g[xx, zz, 16:24, :]
                a0, a1 = pick(same, other), pick(other, same)
                rows = pl.ds(pl.multiple_of(zz * 32 + 8 * xx, 8), 8)
                w13_ref[rows, :HALF] = jnp.where(top, a0, half_swap(a1))
                w13_ref[rows, HALF:] = jnp.where(top, half_swap(a0), a1)
            for pr in range(2):
                b0, b1 = g[2 * pr, zz, 8:16, :], g[2 * pr + 1, zz, 8:16, :]
                rows = pl.ds(pl.multiple_of(zz * 16 + 8 * pr, 8), 8)
                w2_ref[rows, :HALF] = jnp.where(top, b0, half_swap(b1))
                w2_ref[rows, HALF:] = jnp.where(top, half_swap(b0), b1)
            return carry

        lax.fori_loop(0, NZ, step, 0)

    def pieces(w13_ref, w2_ref, p):
        def step(zz, carry):
            for xx in range(NX):
                rows = pl.ds(pl.multiple_of(zz * 32 + 8 * xx, 8), 8)
                first, gate = w13_ref[rows, :HALF], w13_ref[rows, HALF:]
                a0 = jnp.where(top, first, half_swap(gate))
                a1 = jnp.where(top, half_swap(first), gate)
                p[xx, zz, 0:8, :] = pick(a0, a1)
                p[xx, zz, 16:24, :] = pick(a1, a0)
            for pr in range(2):
                rows = pl.ds(pl.multiple_of(zz * 16 + 8 * pr, 8), 8)
                c0, c1 = w2_ref[rows, :HALF], w2_ref[rows, HALF:]
                p[2 * pr, zz, 8:16, :] = jnp.where(top, c0, half_swap(c1))
                p[2 * pr + 1, zz, 8:16, :] = jnp.where(top, half_swap(c0), c1)
            return carry

        lax.fori_loop(0, NZ, step, 0)

    def sum_start(p, rx, sems, xs):
        for d in FAR_FIRST + (0,):
            zp = ahead(z, d, NZ)
            for dx in (2, 1, 3):
                xp = ahead(x, dx, NX)
                send(p.at[xp, zp], rx.at[dx - 1, d], sems.at[0], xs.at[d], tok(z, xp, core))

    def sum_middle(p, rx, total, sems, xs, rza, rzb, zs):
        for d in FAR_FIRST + (0,):
            zp = ahead(z, d, NZ)
            wait(rx.at[:, d], xs.at[d])
            total[d] = (p[x, zp] + rx[0, d]) + (rx[1, d] + rx[2, d])
            if d:
                send(total.at[d, 0:16], rza.at[d - 1], sems.at[1], zs.at[0], tok(zp, x, core))
            send(total.at[d, 16:24], rzb.at[d], sems.at[2], zs.at[1], tok(zp, x, 1 - core))

    def sum_finish(total, rza, rzb, zs):
        wait(rza, zs.at[0])
        wait(rzb, zs.at[1])
        return jnp.concatenate(
            [total[0, 0:16, :] + jnp.sum(rza[...], axis=0), jnp.sum(rzb[...], axis=0)], axis=0
        )

    def sum_sent(p, rza, rzb, sems):
        wait(p.at[0:3], sems.at[0])
        wait(rza, sems.at[1])
        wait(rzb, sems.at[2])

    gather_start(own_w, g_w, agw_s, agw_za, agw_zb)
    for n in range(5):
        share(n)

    wait(k_sib, sib_r.at[0])
    keys = jnp.concatenate([k_in[...], k_sib[...]], axis=0)
    kh[...], kl[...] = split(keys)
    kth[...], ktl[...] = split(keys.T)
    wait(v_sib, sib_r.at[1])
    vh[...], vl[...] = split(jnp.concatenate([v_in[...], v_sib[...]], axis=0))
    wait(r_sib, sib_r.at[4])

    def columns_of(rows8):
        return jnp.broadcast_to(rows8[0:1, :], (HALF, HALF)).T

    rate = jnp.concatenate([columns_of(r_own[...]), columns_of(r_sib[...])], axis=0)

    gather_finish(g_w, agw_s, agw_za, agw_zb, agw_x)
    assemble(g_w, w13, w2)
    w13h[...], w13l[...] = split(w13[...])
    w2h[...], w2l[...] = split(w2[...])

    k_pair, kt_pair, v_pair = (kh[...], kl[...]), (kth[...], ktl[...]), (vh[...], vl[...])
    ug = dot3(k_pair, (w13h[...], w13l[...]), NN)
    inner_v = dot3(v_pair, (w2h[...], w2l[...]), NT)
    u, gate = ug[:, :HALF], ug[:, HALF:]
    sig, s0, s1 = silu_parts(u)
    uq = -rate * s1 * gate
    gq = -rate * s0
    grad_u, grad_g, grad_q = uq * inner_v, gq * inner_v, gq * gate
    grad_ug = jnp.concatenate([grad_u, grad_g], axis=1)
    t13[...] = dot3(kt_pair, split(grad_ug), NN)
    t2[...] = dot3(split(grad_q), v_pair, TN)
    pieces(t13, t2, p_g)
    sum_start(p_g, rx_g, rsg_s, rsg_x)
    c_uq[...] = uq
    c_gq[...] = gq
    c_ug[...] = -rate * s1 * inner_v
    c_uu[...] = -rate * (sig * (1.0 - sig) * (2.0 + u * (1.0 - 2.0 * sig))) * gate * inner_v
    g_ug[...] = grad_ug
    g_q[...] = grad_q
    sum_middle(p_g, rx_g, sum_g, rsg_s, rsg_x, rza_g, rzb_g, rsg_z)

    wait(q_sib, sib_r.at[2])
    wait(oc_sib, sib_r.at[3])
    queries = jnp.concatenate([q_in[...], q_sib[...]], axis=0)
    cot_pair = split(jnp.concatenate([oc_in[...], oc_sib[...]], axis=0))
    w13_pair, w2_pair = (w13h[...], w13l[...]), (w2h[...], w2l[...])
    q_ug = dot3(split(queries), w13_pair, NN)
    d_mixed = dot3(cot_pair, w2_pair, NT)
    q_u, q_gate = q_ug[:, :HALF], q_ug[:, HALF:]
    _, qs0, qs1 = silu_parts(q_u)
    back = split(jnp.concatenate([d_mixed * q_gate * qs1, d_mixed * qs0], axis=1))
    ap13[...] = dot3(split(queries.T), back, NN)
    ap2[...] = dot3(split(qs0 * q_gate), cot_pair, TN)
    part_q[...] = dot3(back, w13_pair, NT)
    send(part_q.at[HALF:], fin_q, fin_s.at[0], fin_r_sem.at[0], sibling)

    def row_sums(a, b):
        prod = a * b
        first = jnp.sum(prod[0:8] + prod[16:24], axis=-1, keepdims=True)
        second = jnp.sum(prod[8:16] + half_swap(prod[8:16]), axis=-1, keepdims=True)
        return jnp.concatenate([first, second, first], axis=0)

    own = own_w[...]
    row_norm = jnp.sqrt(row_sums(own, own) + EPS)
    shifted = own - sum_finish(sum_g, rza_g, rzb_g, rsg_z)
    new_norm = jnp.sqrt(row_sums(shifted, shifted) + EPS)

    @pl.when(y == 3)
    def _():
        to_own(fc_in, z_in)

    @pl.when(y < 3)
    def _():
        wait(z_in, y_sem.at[1])

    incoming = z_in[...]
    inner = row_sums(incoming, shifted)
    d_shifted = row_norm / new_norm * incoming - row_norm * inner / (new_norm * new_norm * new_norm) * shifted
    direct = d_shifted + inner / new_norm * own / row_norm
    own_z[...] = -d_shifted
    gather_start(own_z, g_d, agd_s, agd_za, agd_zb)
    gather_finish(g_d, agd_s, agd_za, agd_zb, agd_x)
    assemble(g_d, d13, d2)
    d13h[...], d13l[...] = split(d13[...])
    d2h[...], d2l[...] = split(d2[...])

    d13_pair, d2_pair = (d13h[...], d13l[...]), (d2h[...], d2l[...])
    ug_dot = dot3(k_pair, d13_pair, NN)
    q_dot = dot3(v_pair, d2_pair, NT)
    u_dot, g_dot = ug_dot[:, :HALF], ug_dot[:, HALF:]
    au = u_dot * c_uu[...] + g_dot * c_ug[...] + q_dot * c_uq[...]
    ag = u_dot * c_ug[...] + q_dot * c_gq[...]
    aq = u_dot * c_uq[...] + g_dot * c_gq[...]
    aug_pair = split(jnp.concatenate([au, ag], axis=1))
    aq_pair = split(aq)
    t13[...] = dot3(kt_pair, aug_pair, NN) + ap13[...]
    t2[...] = dot3(aq_pair, v_pair, TN) + ap2[...]
    pieces(t13, t2, p_z)
    sum_start(p_z, rx_z, rsz_s, rsz_x)
    sum_middle(p_z, rx_z, sum_z, rsz_s, rsz_x, rza_z, rzb_z, rsz_z)

    part_k[...] = dot3(aug_pair, w13_pair, NT) + dot3(split(g_ug[...]), d13_pair, NT)
    send(part_k.at[HALF:], fin_k, fin_s.at[1], fin_r_sem.at[1], sibling)
    part_v[...] = dot3(aq_pair, w2_pair, NN) + dot3(split(g_q[...]), d2_pair, NN)
    send(part_v.at[HALF:], fin_v, fin_s.at[2], fin_r_sem.at[2], sibling)
    each = u_dot * g_ug[:, :HALF] + g_dot * g_ug[:, HALF:] + q_dot * g_q[...]
    part_r[0:8, :] = jnp.broadcast_to(jnp.sum(each[:HALF].T, axis=0, keepdims=True), (8, HALF))
    part_r[8:16, :] = jnp.broadcast_to(jnp.sum(each[HALF:].T, axis=0, keepdims=True), (8, HALF))
    send(part_r.at[8:16], fin_r, fin_s.at[3], fin_r_sem.at[3], sibling)

    rows_now = sum_finish(sum_z, rza_z, rzb_z, rsz_z) + direct
    rows_z[...] = rows_now

    @pl.when(y > 0)
    def _():
        pltpu.make_async_remote_copy(
            src_ref=rows_z, dst_ref=z_in, send_sem=y_sem.at[0], recv_sem=y_sem.at[1],
            device_id=(y - 1, t), device_id_type=pl.DeviceIdType.MESH,
        ).start()

    same, rows2, other = rows_now[0:8], rows_now[8:16], rows_now[16:24]
    one_hot = (hidden_of(row_i) == col_i).astype(F32).astype(BF16)
    a = exact_select(jnp.concatenate([pick(same, other), pick(other, same)], axis=1), one_hot)
    ds_out[0, 0] = a[0:4]
    ds_out[0, 1] = half_swap(a)[0:4]
    ds_out[0, 2, :, :HALF] = rows2[0:4]
    ds_out[0, 2, :, HALF:] = half_swap(rows2)[0:4]

    wait(fin_q, fin_r_sem.at[0])
    dq_out[...] = part_q[:HALF, :] + fin_q[...]
    wait(fin_k, fin_r_sem.at[1])
    dk_out[...] = part_k[:HALF, :] + fin_k[...]
    wait(fin_v, fin_r_sem.at[2])
    dv_out[...] = part_v[:HALF, :] + fin_v[...]
    wait(fin_r, fin_r_sem.at[3])
    dr_out[...] = (part_r[0:1, :] + fin_r[0:1, :]) / r_own[0:1, :]

    for n in range(5):
        wait(pairs[n][1], sib_s.at[n])
    gather_sent(g_w, agw_s)
    sum_sent(p_g, rza_g, rzb_g, rsg_s)
    gather_sent(g_d, agd_s)
    sum_sent(p_z, rza_z, rzb_z, rsz_s)
    for n, ref in enumerate((fin_q, fin_k, fin_v, fin_r)):
        wait(ref, fin_s.at[n])

    @pl.when(y > 0)
    def _():
        wait(z_in, y_sem.at[0])


def per_device(queries, keys, values, rates, states, out_cot, final_cot):
    vmem = pl.BlockSpec(memory_space=pltpu.VMEM)
    f, b, dma = (lambda *s: pltpu.VMEM(s, F32)), (lambda *s: pltpu.VMEM(s, BF16)), (lambda *s: pltpu.SemaphoreType.DMA(s))
    scratch = [f(HALF, D)] * 4 + [f(8, HALF)] * 2
    scratch += [f(24, HALF)] * 4 + [f(16, D)]
    scratch += [f(NX, NZ, 24, HALF)] * 4 + [f(3, NZ, 24, HALF)] * 2
    scratch += [f(7, 16, HALF), f(8, 8, HALF)] * 2 + [f(NZ, 24, HALF)] * 2
    scratch += [f(D, D), f(HALF, D)] * 4
    scratch += [b(D, D)] * 6 + [b(D, D), b(D, D), b(HALF, D), b(HALF, D)] * 2
    scratch += [f(D, HALF)] * 4 + [f(D, D), f(D, HALF)] * 2
    scratch += [f(D, D)] * 3 + [f(16, HALF)] + [f(HALF, D)] * 3 + [f(8, HALF)]
    scratch += [dma(5), dma(5)] + [dma(3), dma(8), dma(8), dma()] * 2
    scratch += [dma(3), dma(8), dma(2)] * 2 + [dma(2), dma(4), dma(4)]
    d_queries, d_keys, d_values, d_rates, d_states = pl.pallas_call(
        kernel,
        out_shape=(
            jax.ShapeDtypeStruct((HALF, D), F32),
            jax.ShapeDtypeStruct((HALF, D), F32),
            jax.ShapeDtypeStruct((HALF, D), F32),
            jax.ShapeDtypeStruct((1, HALF), F32),
            jax.ShapeDtypeStruct((1, 3, 4, D), F32),
        ),
        in_specs=[vmem] * 7,
        out_specs=(vmem,) * 5,
        scratch_shapes=scratch,
        compiler_params=pltpu.CompilerParams(
            collective_id=0, has_side_effects=True, vmem_limit_bytes=40 * 1024 * 1024
        ),
        name="blocks",
    )(queries, keys, values, rates.reshape(1, HALF), states, out_cot, final_cot)
    return d_queries, d_keys, d_values, d_rates.reshape(HALF), d_states


def solution(mesh):
    return jax.shard_map(
        per_device,
        mesh=mesh,
        in_specs=(
            P(("block", "tok"), None),
            P(("block", "tok"), None),
            P(("block", "tok"), None),
            P(("block", "tok")),
            P("block", None, "tok", None),
            P(("block", "tok"), None),
            P(None, "tok", None),
        ),
        out_specs=(
            P(("block", "tok"), None),
            P(("block", "tok"), None),
            P(("block", "tok"), None),
            P(("block", "tok")),
            P("block", None, "tok", None),
        ),
        check_vma=False,
    )
```
